32 devices in a mesh: fsdp: 32 (over z, y, x, core).
Axes of the slice: x: 2, y: 2, z: 4, core: 2. Of those that a mesh axis runs over, the one named last changes fastest.
Arguments:
- grads: bfloat16 [32, 20736, 128], P('fsdp'), may hold values from -15000 to 15000
- params: float32 [20736, 128], P('fsdp'), may hold values from -0.1875 to 0.1875
- moment: float32 [20736, 128], P('fsdp'), may hold values from -6 to 6
- second: float32 [20736, 128], P('fsdp'), may hold values from 0.1 to 4
- teacher: float32 [20736, 128], P('fsdp'), may hold values from -0.1875 to 0.1875
Outputs:
- params_out: float32 [20736, 128], P('fsdp')
- moment_out: float32 [20736, 128], P('fsdp')
- second_out: float32 [20736, 128], P('fsdp')
- teacher_out: float32 [20736, 128], P('fsdp')
- weights_out: bfloat16 [20736, 128], replicated
The draws below stay inside these ranges and needn't reach their ends.
All inputs are finite; a program needn't handle non-finite values.
Results may differ from the reference program's by a relative error of at most 0.001.
Values may be sent and summed in bfloat16 or wider, within the bound.
A program may use at most 128 MiB of HBM per device.

```python
import math
import jax
import jax.numpy as jnp
from jax import lax

D = 1152
ROWS = 20736
N_FSDP = 32


def draw_grads(key, part):
    keys = jax.random.split(jax.random.fold_in(key, 17), 6)
    positions = jnp.arange(ROWS, dtype=jnp.float32)
    rising = jnp.exp(jnp.log(3.0) * positions / ROWS)[:, None]
    row_spread = jnp.exp(jax.random.uniform(keys[0], (ROWS, 1), jnp.float32) * jnp.log(10.0))
    col_spread = jnp.exp(jax.random.uniform(keys[1], (1, 128), jnp.float32) * jnp.log(10.0))
    pairing = jax.random.permutation(keys[5], N_FSDP).astype(jnp.int32)
    block_of_row = (jnp.arange(ROWS, dtype=jnp.int32) // (ROWS // N_FSDP)).astype(jnp.int32)
    boost = jnp.where(block_of_row[None, :] == pairing[:, None], 8.0, 1.0).astype(jnp.float32)[:, :, None]
    noise = jnp.clip(jax.random.normal(keys[4], (N_FSDP, ROWS, 128), jnp.float32), -5.0, 5.0)
    return (noise * boost * rising * row_spread * col_spread).astype(jnp.bfloat16)


def level_of(stream_key, shape, cuts, low, top_value):
    level, own = 1.0, jax.random.fold_in(stream_key, 6)
    for dim, parts in cuts:
        steps = jnp.exp(jax.random.uniform(jax.random.fold_in(own, dim), (parts,), jnp.float32, low / len(cuts), top_value / len(cuts)))
        level = level * jnp.repeat(steps, shape[dim] // parts).reshape([-1 if axis == dim else 1 for axis in range(len(shape))])
    return level


def scatter_about(key, dims, scale, reach, pieces=(), held_as=jnp.bfloat16):
    loudness = level_of(key, dims, pieces, -0.22, 0.18) if pieces else 1.0
    values = jax.random.normal(key, dims, jnp.float32) * scale * loudness
    return jnp.minimum(jnp.maximum(values, -reach), reach).astype(held_as)


def setup_inputs(seed: int = 0) -> dict:
    key_of = jax.random.split(jax.random.key(seed), 6)
    return {
        "grads": draw_grads(jax.random.fold_in(key_of[5], 71), 0),
        "params": scatter_about(key_of[1], (ROWS, 128), D ** -0.5, 0.1875, ((0, 32),), jnp.float32),
        "moment": scatter_about(key_of[2], (ROWS, 128), 1.0, 6.0, ((0, 32),), jnp.float32),
        "second": jnp.clip(jnp.exp(math.log(4.0) - 3.6888794 * jax.random.uniform(key_of[3], (ROWS, 128), jnp.float32) ** level_of(key_of[3], (ROWS, 128), ((0, 32),), -0.2, 0.2)), 0.1, 4.0),
        "teacher": scatter_about(key_of[4], (ROWS, 128), D ** -0.5, 0.1875, ((0, 32),), jnp.float32),
    }


def reference(grads, params, moment, second, teacher):

    def accumulate(total, piece):
        return (total + piece.astype(jnp.float32), None)
    summed, _ = lax.scan(accumulate, jnp.zeros(grads.shape[1:], jnp.float32), grads)
    squares = jnp.sum(summed * summed)
    entries = grads.shape[1] * grads.shape[2]
    factor = 1.0 / jnp.sqrt(squares / jnp.float32(entries) + 1e-06)
    clipped = factor * summed
    moment_out = 0.9 * moment + 0.1 * clipped
    second_out = 0.95 * second + 0.05 * clipped * clipped
    first_fix = 1.0 - 0.9 ** 10
    second_fix = 1.0 - 0.95 ** 10
    update = moment_out / first_fix / (jnp.sqrt(second_out / second_fix) + 1e-08) + 0.1 * params
    params_out = params - 0.001 * update
    teacher_out = 0.9999 * teacher + 0.0001 * params_out
    weights_out = params_out.astype(jnp.bfloat16)
    return (params_out, moment_out, second_out, teacher_out, weights_out)
```

```python
import functools

import jax
import jax.numpy as jnp
from jax import lax
from jax.experimental import pallas as pl
from jax.experimental.pallas import tpu as pltpu
from jax.sharding import PartitionSpec as P

MESH = pl.DeviceIdType.MESH
SHARES = (0.395, 0.765)
NARROW = 0


def adamw(factor, summed, params, moment, second, teacher):
    clipped = factor * summed
    moment_out = 0.9 * moment + 0.1 * clipped
    second_out = 0.95 * second + 0.05 * clipped * clipped
    first_fix = 1.0 - 0.9**10
    second_fix = 1.0 - 0.95**10
    update = moment_out / first_fix / (jnp.sqrt(second_out / second_fix) + 1e-08) + 0.1 * params
    params_out = params - 0.001 * update
    teacher_out = 0.9999 * teacher + 0.0001 * params_out
    return params_out, moment_out, second_out, teacher_out


def plain_body(grads, params, moment, second, teacher):
    summed = lax.psum_scatter(grads[0].astype(jnp.float32), "fsdp", scatter_dimension=0, tiled=True)
    squares = lax.psum(jnp.sum(summed * summed), "fsdp")
    entries = grads.shape[1] * grads.shape[2]
    factor = 1.0 / jnp.sqrt(squares / jnp.float32(entries) + 1e-06)
    outs = adamw(factor, summed, params, moment, second, teacher)
    weights_out = lax.all_gather(outs[0].astype(jnp.bfloat16), "fsdp", axis=0, tiled=True)
    return (*outs, weights_out)


def span(masks):
    held = [0]
    for mask in masks:
        held = held + [j | mask for j in held]
    return held


def kernel(
    n, entries, parts, orders,
    grads, params, moment, second, teacher,
    params_out, moment_out, second_out, teacher_out, weights,
    loc, peer, *rest,
):
    n_parts = len(parts)
    slots = [rest[i * n_parts : (i + 1) * n_parts] for i in range(5)]
    sends, recvs, gathered = slots[0:2], slots[2:4], slots[4]
    (total, square, squares,
     loc_sem, peer_send, peer_recv, rs_send, rs_recv,
     sq_send, sq_recv, ag_send, ag_recv, fw_send, fw_recv, out_sem) = rest[5 * n_parts :]
    half = n // 2
    bits = n.bit_length() - 1
    me = lax.axis_index("fsdp")
    steps = [(1 << i) * (1 - 2 * ((me // (1 << i)) % 2)) for i in range(bits)]

    def at(j):
        where = me
        for i in range(bits):
            if j >> i & 1:
                where = where + steps[i]
        return where

    def remote(src, dst, send, recv, j):
        return pltpu.make_async_remote_copy(
            src_ref=src, dst_ref=dst, send_sem=send, recv_sem=recv,
            device_id=(at(j),), device_id_type=MESH,
        )

    by_need = sorted(range(half), key=lambda j: -(j & 7).bit_count() * half - j)
    peer_copies, loc_copies = {}, {}
    for j in by_need:
        peer_copies[j] = remote(grads.at[at(2 * j + 1)], peer.at[j], peer_send.at[j], peer_recv.at[j], 1)
        peer_copies[j].start()
    for j in by_need:
        loc_copies[j] = pltpu.make_async_copy(grads.at[at(2 * j)], loc.at[j], loc_sem.at[j])
        loc_copies[j].start()

    ready = set()
    rs_copies = {}

    def value(p, j, stage):
        if j not in ready:
            ready.add(j)
            loc_copies[j].wait()
            peer_copies[j].wait_recv()
        rows = pl.ds(*parts[p])
        v = loc[j, rows, :].astype(jnp.float32) + peer[j, rows, :].astype(jnp.float32)
        for earlier, mask in enumerate(orders[p][:stage]):
            rs_copies[p, j | mask].wait_recv()
            v = v + recvs[earlier >= NARROW][p][j | mask].astype(jnp.float32)
        return v

    stages = bits - 1
    for stage in range(stages):
        todo = []
        for p in range(n_parts):
            mask, later = orders[p][stage], orders[p][stage + 1 :]
            todo.append([j | mask for j in reversed(span(later[::-1]))])
        for i in range(len(todo[0])):
            for p in range(n_parts):
                j, mask = todo[p][i], orders[p][stage]
                wide = stage >= NARROW
                source, target = sends[wide][p], recvs[wide][p]
                source[j] = value(p, j, stage).astype(source.dtype)
                rs_copies[p, j] = remote(
                    source.at[j], target.at[j], rs_send.at[p, j], rs_recv.at[p, j], 2 * mask
                )
                rs_copies[p, j].start()

    acc = jnp.zeros(square.shape, jnp.float32)
    for p in range(n_parts):
        v = value(p, 0, stages)
        total[pl.ds(*parts[p]), :] = v
        acc = acc + jnp.sum((v * v).reshape(-1, *square.shape), axis=0)
    square[...] = acc

    def square_copy(k):
        return pltpu.make_async_remote_copy(
            src_ref=square, dst_ref=squares.at[k], send_sem=sq_send.at[k], recv_sem=sq_recv.at[k],
            device_id=(lax.rem(me + k, n),), device_id_type=MESH,
        )

    @pl.loop(1, n)
    def _(k):
        square_copy(k).start()

    @pl.loop(1, n)
    def _(k):
        square_copy(k).wait()

    all_squares = square[...] + jnp.sum(squares[1:], axis=0)
    all_squares = jnp.sum(jnp.sum(all_squares, axis=0, keepdims=True), axis=1, keepdims=True)
    all_squares = jnp.broadcast_to(all_squares, (1, square.shape[1]))
    factor = 1.0 / jnp.sqrt(all_squares / jnp.float32(entries) + 1e-06)

    ag_copies, fw_copies, out_copies = {}, {}, {}

    def forward(p, j, stage):
        mask = orders[p][::-1][stage]
        ag_copies[p, j | mask] = remote(
            gathered[p].at[j], gathered[p].at[j | mask],
            ag_send.at[p, j | mask], ag_recv.at[p, j | mask], 2 * mask,
        )
        ag_copies[p, j | mask].start()

    def settle(p, j):
        rows = pl.ds(*parts[p])
        place = weights.at[at(2 * j), rows]
        fw_copies[p, j] = remote(gathered[p].at[j], place, fw_send.at[p, j], fw_recv.at[p, j], 1)
        fw_copies[p, j].start()
        out_copies[p, j] = pltpu.make_async_copy(gathered[p].at[j], place, out_sem.at[p, j])
        out_copies[p, j].start()

    for p in range(n_parts):
        rows = pl.ds(*parts[p])
        outs = adamw(factor, total[rows, :], params[rows, :], moment[rows, :], second[rows, :], teacher[rows, :])
        gathered[p][0] = outs[0].astype(jnp.bfloat16)
        forward(p, 0, 0)
        params_out[rows, :], moment_out[rows, :], second_out[rows, :], teacher_out[rows, :] = outs
    for stage in range(1, stages):
        for p in range(n_parts):
            forward(p, 0, stage)
    for p in range(n_parts):
        settle(p, 0)
    for stage in range(stages):
        for i in range(1 << stage):
            for p in range(n_parts):
                order = orders[p][::-1]
                j = span(order[:stage])[i] | order[stage]
                ag_copies[p, j].wait_recv()
                for later in range(stage + 1, stages):
                    forward(p, j, later)
                settle(p, j)

    for copy in fw_copies.values():
        copy.wait()
    for copy in out_copies.values():
        copy.wait()
    for copies in (peer_copies, rs_copies, ag_copies):
        for copy in copies.values():
            copy.wait_send()


def split(rows):
    first = int(rows * SHARES[0]) // 16 * 16
    second = int(rows * SHARES[1]) // 16 * 16
    return ((0, first), (first, second - first), (second, rows - second))


def fast_body(n, grads, params, moment, second, teacher):
    rows, lanes = params.shape
    half = n // 2
    parts = split(rows)
    masks = [1 << i for i in range(n.bit_length() - 2)]
    orders = (
        tuple(masks),
        (masks[1], masks[0], *masks[2:]),
        (*masks[2:], masks[0], masks[1]),
    )
    shard = jax.ShapeDtypeStruct((rows, lanes), jnp.float32)
    vmem, hbm = pl.BlockSpec(memory_space=pltpu.VMEM), pl.BlockSpec(memory_space=pl.ANY)
    narrow, wide = ([pltpu.VMEM((half, size, lanes), t) for _, size in parts] for t in (jnp.bfloat16, jnp.float32))
    dma = pltpu.SemaphoreType.DMA
    per_part = dma((len(parts), half))
    outs = pl.pallas_call(
        functools.partial(kernel, n, grads.shape[1] * lanes, parts, orders),
        out_shape=(shard,) * 4 + (jax.ShapeDtypeStruct((n, rows, lanes), jnp.bfloat16),),
        in_specs=[hbm, vmem, vmem, vmem, vmem],
        out_specs=(vmem,) * 4 + (hbm,),
        scratch_shapes=[pltpu.VMEM((half, rows, lanes), jnp.bfloat16)] * 2
        + narrow + wide + narrow + wide + narrow
        + [
            pltpu.VMEM((rows, lanes), jnp.float32),
            pltpu.VMEM((8, lanes), jnp.float32),
            pltpu.VMEM((n, 8, lanes), jnp.float32),
            dma((half,)), dma((half,)), dma((half,)),
            per_part, per_part,
            dma((n,)), dma((n,)),
            per_part, per_part, per_part, per_part, per_part,
        ],
        compiler_params=pltpu.CompilerParams(has_side_effects=True, vmem_limit_bytes=40 * 1024 * 1024),
    )(grads.reshape(n, rows, lanes), params, moment, second, teacher)
    return (*outs[:4], outs[4].reshape(n * rows, lanes))


def body(n, grads, params, moment, second, teacher):
    if n & (n - 1) == 0 and 16 <= n <= 64 and params.shape[0] % 8 == 0 and params.shape[0] >= 128:
        return fast_body(n, grads, params, moment, second, teacher)
    return plain_body(grads, params, moment, second, teacher)


def solution(mesh):
    in_specs = (
        P("fsdp", None, None),
        P("fsdp", None),
        P("fsdp", None),
        P("fsdp", None),
        P("fsdp", None),
    )
    out_specs = (P("fsdp", None), P("fsdp", None), P("fsdp", None), P("fsdp", None), P())
    run = functools.partial(body, mesh.shape["fsdp"])
    return jax.shard_map(run, mesh=mesh, in_specs=in_specs, out_specs=out_specs, check_vma=False)
```

```python
import functools

import jax
import jax.numpy as jnp
from jax import lax
from jax.experimental import pallas as pl
from jax.experimental.pallas import tpu as pltpu
from jax.sharding import PartitionSpec as P

MESH = pl.DeviceIdType.MESH
SHARES = (0.395, 0.765)
VMEM_GRANT = 67000000
PIECES = 8


def adamw(factor, summed, params, moment, second, teacher):
    clipped = factor * summed
    moment_out = 0.9 * moment + 0.1 * clipped
    second_out = 0.95 * second + 0.05 * clipped * clipped
    first_fix = 1.0 - 0.9**10
    second_fix = 1.0 - 0.95**10
    update = moment_out / first_fix / (jnp.sqrt(second_out / second_fix) + 1e-08) + 0.1 * params
    params_out = params - 0.001 * update
    teacher_out = 0.9999 * teacher + 0.0001 * params_out
    return params_out, moment_out, second_out, teacher_out


def plain_body(grads, params, moment, second, teacher):
    summed = lax.psum_scatter(grads[0].astype(jnp.float32), "fsdp", scatter_dimension=0, tiled=True)
    squares = lax.psum(jnp.sum(summed * summed), "fsdp")
    entries = grads.shape[1] * grads.shape[2]
    factor = 1.0 / jnp.sqrt(squares / jnp.float32(entries) + 1e-06)
    outs = adamw(factor, summed, params, moment, second, teacher)
    weights_out = lax.all_gather(outs[0].astype(jnp.bfloat16), "fsdp", axis=0, tiled=True)
    return (*outs, weights_out)


def span(masks):
    held = [0]
    for mask in masks:
        held = held + [j | mask for j in held]
    return held


def kernel(
    n, entries, parts, orders,
    grads, params, moment, second, teacher,
    params_out, moment_out, second_out, teacher_out, weights,
    state, loc, peer, *rest,
):
    n_parts = len(parts)
    sends, recvs, gathered = rest[:n_parts], rest[n_parts : 2 * n_parts], rest[2 * n_parts : 3 * n_parts]
    (total, square, squares,
     state_sem, loc_sem, peer_send, peer_recv, rs_send, rs_recv,
     sq_send, sq_recv, ag_send, ag_recv, fw_send, fw_recv, out_sem) = rest[3 * n_parts :]
    half = n // 2
    bits = n.bit_length() - 1
    me = lax.axis_index("fsdp")
    steps = [(1 << i) * (1 - 2 * ((me // (1 << i)) % 2)) for i in range(bits)]

    def at(j):
        where = me
        for i in range(bits):
            if j >> i & 1:
                where = where + steps[i]
        return where

    def remote(src, dst, send, recv, j):
        return pltpu.make_async_remote_copy(
            src_ref=src, dst_ref=dst, send_sem=send, recv_sem=recv,
            device_id=(at(j),), device_id_type=MESH,
        )

    by_need = sorted(range(half), key=lambda j: -(j & 7).bit_count() * half - j)
    peer_copies, loc_copies = {}, {}
    for j in by_need:
        peer_copies[j] = remote(grads.at[at(2 * j + 1)], peer.at[j], peer_send.at[j], peer_recv.at[j], 1)
        peer_copies[j].start()
    for j in by_need:
        loc_copies[j] = pltpu.make_async_copy(grads.at[at(2 * j)], loc.at[j], loc_sem.at[j])
        loc_copies[j].start()

    ready = set()
    rs_copies = {}

    def value(p, j, stage):
        if j not in ready:
            ready.add(j)
            loc_copies[j].wait()
            peer_copies[j].wait_recv()
        rows = pl.ds(*parts[p])
        v = loc[j, rows, :].astype(jnp.float32) + peer[j, rows, :].astype(jnp.float32)
        for mask in orders[p][:stage]:
            rs_copies[p, j | mask].wait_recv()
            v = v + recvs[p][j | mask]
        return v

    state_copies = [
        pltpu.make_async_copy(ref, state.at[i], state_sem.at[i])
        for i, ref in enumerate((params, moment, second, teacher))
    ]
    for copy in state_copies:
        copy.start()

    stages = bits - 1
    for stage in range(stages):
        todo = []
        for p in range(n_parts):
            mask, later = orders[p][stage], orders[p][stage + 1 :]
            todo.append([j | mask for j in reversed(span(later[::-1]))])
        for i in range(len(todo[0])):
            for p in range(n_parts):
                j, mask = todo[p][i], orders[p][stage]
                source, target = sends[p], recvs[p]
                source[j] = value(p, j, stage)
                rs_copies[p, j] = remote(
                    source.at[j], target.at[j], rs_send.at[p, j], rs_recv.at[p, j], 2 * mask
                )
                rs_copies[p, j].start()

    acc = jnp.zeros(square.shape, jnp.float32)
    for p in range(n_parts):
        v = value(p, 0, stages)
        total[pl.ds(*parts[p]), :] = v
        acc = acc + jnp.sum((v * v).reshape(-1, *square.shape), axis=0)
    square[...] = acc

    def square_copy(k):
        return pltpu.make_async_remote_copy(
            src_ref=square, dst_ref=squares.at[k], send_sem=sq_send.at[k], recv_sem=sq_recv.at[k],
            device_id=(lax.rem(me + k, n),), device_id_type=MESH,
        )

    @pl.loop(1, n)
    def _(k):
        square_copy(k).start()

    @pl.loop(1, n)
    def _(k):
        square_copy(k).wait()

    all_squares = square[...] + jnp.sum(squares[1:], axis=0)
    all_squares = jnp.sum(jnp.sum(all_squares, axis=0, keepdims=True), axis=1, keepdims=True)
    all_squares = jnp.broadcast_to(all_squares, (1, square.shape[1]))
    factor = 1.0 / jnp.sqrt(all_squares / jnp.float32(entries) + 1e-06)

    ag_copies, fw_copies, out_copies = {}, {}, {}

    def forward(p, j, stage):
        mask = orders[p][::-1][stage]
        ag_copies[p, j | mask] = remote(
            gathered[p].at[j], gathered[p].at[j | mask],
            ag_send.at[p, j | mask], ag_recv.at[p, j | mask], 2 * mask,
        )
        ag_copies[p, j | mask].start()

    def settle(p, j):
        rows = pl.ds(*parts[p])
        place = weights.at[at(2 * j), rows]
        fw_copies[p, j] = remote(gathered[p].at[j], place, fw_send.at[p, j], fw_recv.at[p, j], 1)
        fw_copies[p, j].start()
        out_copies[p, j] = pltpu.make_async_copy(gathered[p].at[j], place, out_sem.at[p, j])
        out_copies[p, j].start()

    for copy in state_copies:
        copy.wait()
    for p in range(n_parts):
        rows = pl.ds(*parts[p])
        outs = adamw(factor, total[rows, :], *(state[i, rows, :] for i in range(4)))
        gathered[p][0] = outs[0].astype(jnp.bfloat16)
        forward(p, 0, 0)
        params_out[rows, :], moment_out[rows, :], second_out[rows, :], teacher_out[rows, :] = outs
    for stage in range(1, stages):
        for p in range(n_parts):
            forward(p, 0, stage)
    for p in range(n_parts):
        settle(p, 0)
    for stage in range(stages):
        for i in range(1 << stage):
            for p in range(n_parts):
                order = orders[p][::-1]
                j = span(order[:stage])[i] | order[stage]
                ag_copies[p, j].wait_recv()
                for later in range(stage + 1, stages):
                    forward(p, j, later)
                settle(p, j)

    for copy in fw_copies.values():
        copy.wait()
    for copy in out_copies.values():
        copy.wait()
    for copies in (peer_copies, rs_copies, ag_copies):
        for copy in copies.values():
            copy.wait_send()


def land(*refs):
    sources, places, held, (in_sem, out_sem) = refs[:5], refs[5:10], refs[10:15], refs[15:]
    jobs = [(i, pl.ds(0, sources[i].shape[0])) for i in range(4)]
    size = sources[4].shape[0] // PIECES // 16 * 16
    for k in range(PIECES):
        jobs.append((4, pl.ds(k * size, size if k < PIECES - 1 else sources[4].shape[0] - k * size)))
    jobs = jobs[4:] + jobs[:4]
    incoming = [
        pltpu.make_async_copy(sources[i].at[rows], held[i].at[rows], in_sem.at[k])
        for k, (i, rows) in enumerate(jobs)
    ]
    outgoing = [
        pltpu.make_async_copy(held[i].at[rows], places[i].at[rows], out_sem.at[k])
        for k, (i, rows) in enumerate(jobs)
    ]
    for copy in incoming:
        copy.start()
    for copy, out in zip(incoming, outgoing):
        copy.wait()
        out.start()
    for out in outgoing:
        out.wait()


def split(rows):
    first = int(rows * SHARES[0]) // 16 * 16
    second = int(rows * SHARES[1]) // 16 * 16
    return ((0, first), (first, second - first), (second, rows - second))


def fast_body(n, grads, params, moment, second, teacher):
    rows, lanes = params.shape
    half = n // 2
    parts = split(rows)
    masks = [1 << i for i in range(n.bit_length() - 2)]
    orders = (
        tuple(masks),
        (masks[1], masks[0], *masks[2:]),
        (*masks[2:], masks[0], masks[1]),
    )
    shard = jax.ShapeDtypeStruct((rows, lanes), jnp.float32)
    vmem, hbm, anywhere = (pl.BlockSpec(memory_space=space) for space in (pltpu.VMEM, pltpu.HBM, pl.ANY))
    narrow, wide = ([pltpu.VMEM((half, size, lanes), t) for _, size in parts] for t in (jnp.bfloat16, jnp.float32))
    dma = pltpu.SemaphoreType.DMA
    per_part = dma((len(parts), half))
    outs = pl.pallas_call(
        functools.partial(kernel, n, grads.shape[1] * lanes, parts, orders),
        out_shape=(shard,) * 4 + (jax.ShapeDtypeStruct((n, rows, lanes), jnp.bfloat16),),
        in_specs=[anywhere] + [hbm] * 4,
        out_specs=(vmem,) * 4 + (anywhere,),
        scratch_shapes=[pltpu.VMEM((4, rows, lanes), jnp.float32)]
        + [pltpu.VMEM((half, rows, lanes), jnp.bfloat16)] * 2
        + wide + wide + narrow
        + [
            pltpu.VMEM((rows, lanes), jnp.float32),
            pltpu.VMEM((8, lanes), jnp.float32),
            pltpu.VMEM((n, 8, lanes), jnp.float32),
            dma((4,)), dma((half,)), dma((half,)), dma((half,)),
            per_part, per_part,
            dma((n,)), dma((n,)),
            per_part, per_part, per_part, per_part, per_part,
        ],
        compiler_params=pltpu.CompilerParams(has_side_effects=True, vmem_limit_bytes=VMEM_GRANT),
    )(grads.reshape(n, rows, lanes), params, moment, second, teacher)
    shapes = (shard,) * 4 + (jax.ShapeDtypeStruct((n * rows, lanes), jnp.bfloat16),)
    return pl.pallas_call(
        land,
        out_shape=shapes,
        in_specs=[anywhere] * 5,
        out_specs=(anywhere,) * 5,
        scratch_shapes=[pltpu.VMEM(s.shape, s.dtype) for s in shapes] + [dma((4 + PIECES,))] * 2,
        compiler_params=pltpu.CompilerParams(vmem_limit_bytes=VMEM_GRANT),
    )(*outs[:4], outs[4].reshape(n * rows, lanes))


def body(n, grads, params, moment, second, teacher):
    if n & (n - 1) == 0 and 16 <= n <= 64 and params.shape[0] % 8 == 0 and params.shape[0] >= 128:
        return fast_body(n, grads, params, moment, second, teacher)
    return plain_body(grads, params, moment, second, teacher)


def solution(mesh):
    in_specs = (
        P("fsdp", None, None),
        P("fsdp", None),
        P("fsdp", None),
        P("fsdp", None),
        P("fsdp", None),
    )
    out_specs = (P("fsdp", None), P("fsdp", None), P("fsdp", None), P("fsdp", None), P())
    run = functools.partial(body, mesh.shape["fsdp"])
    return jax.shard_map(run, mesh=mesh, in_specs=in_specs, out_specs=out_specs, check_vma=False)
```
